32 devices in a mesh: gx: 4 (over y, core), gy: 4 (over z), gz: 2 (over x).
Axes of the slice: x: 2, y: 2, z: 4, core: 2. Of those that a mesh axis runs over, the one named last changes fastest.
Arguments:
- tokens: bfloat16 [256, 7168], P(('gx', 'gy', 'gz')), may hold values from -6 to 6
- expert_ids: int32 [256, 8], P(('gx', 'gy', 'gz')), may hold values from 0 to 15, as said below
- slot_ids: int32 [256, 8], P(('gx', 'gy', 'gz')), may hold values from 0 to 7, as said below
- route_weight: bfloat16 [256, 8], P(('gx', 'gy', 'gz')), may hold values from 0.099609375 to 0.59765625
- gate_weight: bfloat16 [16, 7168, 2048], P(('gx', 'gy'), None, 'gz'), may hold values from -0.0625 to 0.0625
- up_weight: bfloat16 [16, 7168, 2048], P(('gx', 'gy'), None, 'gz'), may hold values from -0.0625 to 0.0625
- down_weight: bfloat16 [16, 2048, 7168], P(('gx', 'gy'), 'gz'), may hold values from -0.125 to 0.125
- expert_bias: float32 [16], replicated, may hold values from -3 to 3
Outputs:
- combined: bfloat16 [256, 7168], P(('gx', 'gy', 'gz'))
- expert_load: int32 [16], replicated
- new_bias: float32 [16], replicated
The draws below stay inside these ranges and needn't reach their ends.
Inputs may be any that keep to these rules, and one draw needn't show every extreme that they name: `expert_ids`: the 8 experts of a token are different. Among the 8 tokens of one device no expert is named more than 8 times; one expert is named by every token of every device. `slot_ids`: for each device and expert, the routes of that device's tokens to that expert hold different slots.
All inputs are finite; a program needn't handle non-finite values.
Results may differ from the reference program's by a relative error of at most 0.015.
Values may be sent and summed in bfloat16 or wider, within the bound.
A program may use at most 128 MiB of HBM per device.

```python
import jax
import jax.numpy as jnp
from jax import lax

D = 7168
FF = 2048
TOPK = 8
TOK_DEV = 8
PLACE_LIMIT = 8
HID_PARTS = 2
FF_PART = 1024
EXPERTS = 16
TOKENS = 256


def route_tables(key):
    base = jax.random.fold_in(key, 31)
    keys = jax.random.split(base, 5)
    blocks = TOKENS // TOK_DEV
    expert_index = jnp.arange(EXPERTS, dtype=jnp.int32)
    roots = jax.random.randint(keys[0], (EXPERTS,), 0, 64)
    favorite = jax.random.randint(keys[1], (), 0, EXPERTS)
    overfull_mask = roots * roots + 100000 * (expert_index == favorite).astype(jnp.int32)
    block_index = jnp.arange(blocks, dtype=jnp.int32)
    window_start = block_index * EXPERTS // blocks
    within_window = (expert_index[None, :] - window_start[:, None]) % EXPERTS < EXPERTS // 2
    window_reward = 4000 * within_window.astype(jnp.int32)
    random_noise = jax.random.randint(keys[2], (blocks, TOK_DEV, EXPERTS), 0, 2000)
    cyclic_offset = jax.random.randint(keys[3], (blocks, TOK_DEV), 0, EXPERTS)
    shuffle = jax.random.randint(keys[4], (blocks, EXPERTS, PLACE_LIMIT), 0, 1 << 20) * PLACE_LIMIT + jnp.arange(PLACE_LIMIT, dtype=jnp.int32)
    rankings = jnp.argsort(shuffle, axis=-1, stable=True).astype(jnp.int32)

    def lone_portion(jitter_entries, shifted_entries, preference_order, interval_extra_vector):

        def advance(places_filled, inputs):
            present_jitter, rotation_now = inputs
            gating_scores = jnp.where(places_filled >= PLACE_LIMIT, -1, overfull_mask + interval_extra_vector + present_jitter)
            keyed = gating_scores * EXPERTS + (expert_index + rotation_now) % EXPERTS
            _, chosen = lax.top_k(keyed, TOPK)
            chosen = chosen.astype(jnp.int32)
            arrival = places_filled[chosen]
            slot_now = preference_order[chosen, arrival]
            hits_now = jnp.sum((chosen[:, None] == expert_index[None, :]).astype(jnp.int32), axis=0)
            return (places_filled + hits_now, (chosen, slot_now))
        _, (selected_experts, slot_buffer) = lax.scan(advance, jnp.zeros((EXPERTS,), jnp.int32), (jitter_entries, shifted_entries))
        return (selected_experts, slot_buffer)
    selected_experts, slot_buffer = jax.vmap(lone_portion)(random_noise, cyclic_offset, rankings, window_reward)
    return (selected_experts.reshape(TOKENS, TOPK).astype(jnp.int32), slot_buffer.reshape(TOKENS, TOPK).astype(jnp.int32))


def draw_expert_ids(key, part):
    return route_tables(key)[0]


def draw_slot_ids(key, part):
    return route_tables(key)[1]


def block_levels(key, extent, cuts, low, largest):
    def one(dim, parts):
        steps = jax.random.uniform(jax.random.fold_in(jax.random.fold_in(key, 6), dim), (parts,), jnp.float32, low / len(cuts), largest / len(cuts))
        return jnp.repeat(jnp.exp(steps), extent[dim] // parts).reshape((-1,) + (1,) * (len(extent) - dim - 1))

    factor_of = one(*cuts[0])
    for cut in cuts[1:]:
        factor_of = factor_of * one(*cut)
    return factor_of


def normal_values(rng, shape, spread, reach, cuts=(), kind=jnp.bfloat16):
    loudness = block_levels(rng, shape, cuts, -0.22, 0.18) if cuts else 1.0
    result = jax.random.normal(rng, shape, jnp.float32) * spread * loudness
    return jnp.minimum(jnp.maximum(result, -reach), reach).astype(kind)


def setup_inputs(seed: int = 0) -> dict:
    streams_of = jax.random.split(jax.random.key(seed), 9)
    tokens = normal_values(streams_of[0], (TOKENS, D), 1.0, 6.0, ((0, 32),))
    expert_ids = draw_expert_ids(jax.random.fold_in(streams_of[8], 71), 0)
    slot_ids = draw_slot_ids(jax.random.fold_in(streams_of[8], 71), 0)
    route_weight = jnp.clip(0.099609375 + 0.49804688 * jax.random.uniform(streams_of[3], (TOKENS, TOPK), jnp.float32) ** block_levels(streams_of[3], (TOKENS, TOPK), ((0, 32),), -0.2, 0.2), 0.099609375, 0.59765625).astype(jnp.bfloat16)
    gate_weight = normal_values(streams_of[4], (EXPERTS, D, FF), D ** -0.5, 0.0625, ((0, 16), (2, 2)))
    up_weight = normal_values(streams_of[5], (EXPERTS, D, FF), D ** -0.5, 0.0625, ((0, 16), (2, 2)))
    down_weight = normal_values(streams_of[6], (EXPERTS, FF, D), FF ** -0.5, 0.125, ((0, 16), (1, 2)))
    expert_bias = normal_values(streams_of[7], (EXPERTS,), 0.5, 3.0, (), jnp.float32)
    return dict(tokens=tokens, expert_ids=expert_ids, slot_ids=slot_ids, route_weight=route_weight, gate_weight=gate_weight, up_weight=up_weight, down_weight=down_weight, expert_bias=expert_bias)


bias_rate = 0.001


def reference(tokens, expert_ids, slot_ids, route_weight, gate_weight, up_weight, down_weight, expert_bias):
    sources = TOKENS // TOK_DEV
    source = jnp.broadcast_to((jnp.arange(TOKENS, dtype=jnp.int32) // TOK_DEV)[:, None], (TOKENS, TOPK))
    buffer = jnp.zeros((EXPERTS, sources, PLACE_LIMIT, D), jnp.bfloat16)
    buffer = buffer.at[expert_ids, source, slot_ids].set(jnp.broadcast_to(tokens[:, None, :], (TOKENS, TOPK, D)))

    def run_expert(inputs):
        rows_in, gate_mat, up_mat, down_mat = inputs
        flat_rows = rows_in.reshape(sources * PLACE_LIMIT, D)
        gate_act = jnp.dot(flat_rows, gate_mat, preferred_element_type=jnp.float32)
        up_act = jnp.dot(flat_rows, up_mat, preferred_element_type=jnp.float32)
        hidden = (jax.nn.silu(gate_act) * up_act).astype(jnp.bfloat16)
        total = jnp.zeros((sources * PLACE_LIMIT, D), jnp.float32)
        for segment in range(HID_PARTS):
            begin_at = segment * FF_PART
            partial_out = jnp.dot(hidden[:, begin_at:begin_at + FF_PART], down_mat[begin_at:begin_at + FF_PART], preferred_element_type=jnp.float32).astype(jnp.bfloat16)
            total = total + lax.optimization_barrier(partial_out).astype(jnp.float32)
        return total.astype(jnp.bfloat16).reshape(sources, PLACE_LIMIT, D)

    results = lax.map(run_expert, (buffer, gate_weight, up_weight, down_weight))
    selected_experts = results[expert_ids, source, slot_ids]
    combined = jnp.sum(route_weight.astype(jnp.float32)[:, :, None] * selected_experts.astype(jnp.float32), axis=1).astype(jnp.bfloat16)
    counts = jnp.sum((expert_ids[:, :, None] == jnp.arange(EXPERTS, dtype=jnp.int32)).astype(jnp.int32), axis=(0, 1))
    mean_load = TOKENS * TOPK // EXPERTS
    new_bias = expert_bias + bias_rate * jnp.sign((mean_load - counts).astype(jnp.float32))
    return (combined, counts, new_bias)
```

```python
import jax
import jax.numpy as jnp
from jax import lax
from jax.experimental import pallas as pl
from jax.experimental.pallas import tpu as pltpu
from jax.sharding import PartitionSpec as P

PLACE_LIMIT = 8


bias_rate = 0.001


def pack_rows(targets, tokens, row_total):
    selection = jnp.any(
        targets[None, :, :] == jnp.arange(row_total, dtype=jnp.int32)[:, None, None], axis=2
    )
    return jnp.dot(
        selection.astype(jnp.bfloat16), tokens, preferred_element_type=jnp.float32
    ).astype(jnp.bfloat16)


def send_rows(buffer):
    arrived = lax.all_to_all(buffer, ("gx", "gy", "gz"), split_axis=1, concat_axis=1, tiled=True)
    return arrived


def return_rows(buffer):
    arrived = lax.all_to_all(buffer, ("gx", "gy", "gz"), split_axis=1, concat_axis=1, tiled=True)
    return arrived


def slot_body(
    tokens, expert_ids, slot_ids, route_weight, gate_weight, up_weight, down_weight, expert_bias
):
    experts = lax.axis_size("gx") * lax.axis_size("gy")
    gz_parts = lax.axis_size("gz")
    devices = experts * gz_parts
    tok_rows, model_width = tokens.shape
    route_count = expert_ids.shape[1]
    capacity = PLACE_LIMIT
    slot_share = capacity // gz_parts
    expert_index = jnp.arange(experts, dtype=jnp.int32)
    local_hits = jnp.sum((expert_ids[:, :, None] == expert_index).astype(jnp.int32), axis=(0, 1))
    expert_load = lax.psum(local_hits, ("gx", "gy", "gz"))
    mean_load = tok_rows * devices * route_count // experts
    new_bias = expert_bias + bias_rate * jnp.sign((mean_load - expert_load).astype(jnp.float32))
    back_rows = slot_ids % slot_share * devices + expert_ids * gz_parts + slot_ids // slot_share
    packed = pack_rows(slot_ids * experts + expert_ids, tokens, capacity * experts)
    repeated = jnp.broadcast_to(
        packed.reshape(capacity, experts, 1, model_width),
        (capacity, experts, gz_parts, model_width),
    )
    received = send_rows(repeated.reshape(capacity, devices, model_width))
    gate_mat = gate_weight[0]
    up_mat = up_weight[0]
    down_mat = down_weight[0]
    flat_rows = received.reshape(slot_share * lax.axis_size("gz") * devices, model_width)
    gate_act = jnp.dot(flat_rows, gate_mat, preferred_element_type=jnp.float32)
    up_act = jnp.dot(flat_rows, up_mat, preferred_element_type=jnp.float32)
    hidden = (jax.nn.silu(gate_act) * up_act).astype(jnp.bfloat16)
    partial_out = jnp.dot(hidden, down_mat, preferred_element_type=jnp.float32)
    summed = lax.psum_scatter(
        partial_out.reshape(slot_share * lax.axis_size("gz"), devices, model_width).astype(
            jnp.bfloat16
        ),
        "gz",
        scatter_dimension=0,
        tiled=True,
    )
    answers = return_rows(summed)
    flat_answers = answers.reshape(slot_share * devices, model_width)
    spread = jnp.where(
        back_rows[:, :, None] == jnp.arange(slot_share * devices, dtype=jnp.int32),
        route_weight.astype(jnp.float32)[:, :, None],
        0.0,
    )
    mixing = jnp.sum(spread, axis=1).astype(jnp.bfloat16)
    combined = jnp.dot(mixing, flat_answers, preferred_element_type=jnp.float32).astype(
        jnp.bfloat16
    )
    return (combined, expert_load, new_bias)


PAIR = 1024
HALF = PAIR // 2
TILE = 256
LANES = 128
MESH = pl.DeviceIdType.MESH


def layer_kernel(
    tok_ref, ids_ref, rw_ref, wg_hbm, wu_hbm, wd_hbm,
    out_ref, cnt_ref,
    wg, wu, wd, gath, meta, xbuf, acc_g, acc_u, hid,
    s0, r1, s1, r2, s2, r3, s3, r4,
    w_sem, gz_s, gz_r, g1_s, g1_r, g2_s, g2_r, g3_s, g3_r,
    c1_s, c1_r, c2_s, c2_r, c3_s, c3_r, c4_s, c4_r,
):
    f32, bf16 = jnp.float32, jnp.bfloat16
    gx, z, x = lax.axis_index("gx"), lax.axis_index("gy"), lax.axis_index("gz")
    nz = lax.axis_size("gy")
    experts = lax.axis_size("gx") * nz
    y, core = gx // 2, gx % 2
    rows = tok_ref.shape[0]
    total = gath.shape[1] * gath.shape[2] * gath.shape[3] * nz * rows
    ff = hid.shape[1]
    pairs = gath.shape[0] // 2
    sib = (y * 2 + (1 - core), z, x)
    ypeer = ((1 - y) * 2 + core, z, x)
    xpeer = (gx, z, 1 - x)

    def zpeer(d):
        return (gx, lax.rem(z + d, nz), x)

    def wcopies(j):
        span = pl.ds(pl.multiple_of(j * PAIR, PAIR), PAIR)
        return (
            pltpu.make_async_copy(wg_hbm.at[0, span, :], wg.at[j], w_sem.at[0, j]),
            pltpu.make_async_copy(wu_hbm.at[0, span, :], wu.at[j], w_sem.at[1, j]),
        )

    def dcopy(j):
        span = pl.ds(pl.multiple_of(j * PAIR, PAIR), PAIR)
        return pltpu.make_async_copy(wd_hbm.at[0, :, span], wd.at[j], w_sem.at[2, j])

    def start_gate(j, carry):
        for c in wcopies(j):
            c.start()
        return carry

    def start_down(j, carry):
        dcopy(j).start()
        return carry

    lax.fori_loop(0, pairs, start_gate, 0)
    lax.fori_loop(0, pairs, start_down, 0)

    ids = ids_ref[...]
    rw = rw_ref[...].astype(f32)
    lane = lax.broadcasted_iota(jnp.int32, (rows, LANES), 1)
    table = jnp.zeros((rows, LANES), f32)
    for k in range(ids.shape[1]):
        col = ids[:, k:k + 1]
        table = table + jnp.where(lane == col, rw[:, k:k + 1], 0.0)
        table = table + jnp.where(lane == col + experts, 1.0, 0.0)
    meta[core, y, x, z] = table.astype(bf16)

    barrier = pltpu.get_barrier_semaphore()
    peers = [sib, ypeer, xpeer] + [zpeer(d) for d in range(1, nz)]
    for peer in peers:
        pl.semaphore_signal(barrier, inc=1, device_id=peer, device_id_type=MESH)
    pl.semaphore_wait(barrier, len(peers))

    def remote(src, dst, ssem, rsem, dev):
        return pltpu.make_async_remote_copy(
            src_ref=src, dst_ref=dst, send_sem=ssem, recv_sem=rsem,
            device_id=dev, device_id_type=MESH,
        )

    last = pairs * 2

    def view(q):
        return meta if q is None else gath.at[q]

    def semi(q):
        return last if q is None else q

    def cols(q):
        return pl.ds(pl.multiple_of(q * HALF, HALF), HALF)

    def gz(q, d, inn=False):
        buf = view(q)
        own = buf.at[core, y, x, z]
        src = meta.at[core, y, x, z] if q is None else tok_ref.at[:, cols(q)]
        dst = buf.at[core, y, x, lax.rem(z - d + nz, nz)] if inn else own
        return remote(src, dst, gz_s.at[semi(q), d - 1], gz_r.at[semi(q), d - 1], zpeer(d))

    def own_copy(q):
        return pltpu.make_async_copy(
            tok_ref.at[:, cols(q)], gath.at[q, core, y, x, z], w_sem.at[3, q]
        )

    def g1(q, par, inn=False):
        buf = view(q)
        src = buf.at[core, y, x]
        if par == 0:
            dst = buf.at[core, y, 1 - x] if inn else src
            dev = xpeer
        else:
            dst = buf.at[core, 1 - y, x] if inn else src
            dev = ypeer
        return remote(src, dst, g1_s.at[semi(q)], g1_r.at[semi(q)], dev)

    def g2(q, par, inn=False):
        buf = view(q)
        if par == 0:
            src = buf.at[core, y]
            dst = buf.at[core, 1 - y] if inn else src
            dev = ypeer
        else:
            src = buf.at[core, :, x]
            dst = buf.at[core, :, 1 - x] if inn else src
            dev = xpeer
        return remote(src, dst, g2_s.at[semi(q)], g2_r.at[semi(q)], dev)

    def g3(q, inn=False):
        buf = view(q)
        src = buf.at[core]
        dst = buf.at[1 - core] if inn else src
        return remote(src, dst, g3_s.at[semi(q)], g3_r.at[semi(q)], sib)

    for d in range(1, nz):
        gz(None, d).start()

    def send_z(i, carry):
        for par in (0, 1):
            q = 2 * i + par
            for d in range(1, nz):
                gz(q, d).start()
            own_copy(q).start()
        return carry

    lax.fori_loop(0, pairs, send_z, 0)

    for d in range(1, nz):
        gz(None, d, True).wait_recv()
    g1(None, 0).start()

    acc_g[...] = jnp.zeros_like(acc_g)
    acc_u[...] = jnp.zeros_like(acc_u)

    def gather_step(i, carry):
        @pl.when(i < pairs)
        def _():
            for par in (0, 1):
                q = 2 * i + par
                own_copy(q).wait()
                for d in range(1, nz):
                    gz(q, d, True).wait_recv()
                g1(q, par).start()

        @pl.when(i == 0)
        def _():
            g1(None, 0, True).wait_recv()
            g2(None, 0).start()

        @pl.when((i >= 1) & (i < pairs + 1))
        def _():
            for par in (0, 1):
                q = 2 * (i - 1) + par
                g1(q, par, True).wait_recv()
                g2(q, par).start()

        @pl.when(i == 1)
        def _():
            g2(None, 0, True).wait_recv()
            g3(None).start()

        @pl.when((i >= 2) & (i < pairs + 2))
        def _():
            for par in (0, 1):
                q = 2 * (i - 2) + par
                g2(q, par, True).wait_recv()
                g3(q).start()

        @pl.when(i >= 3)
        def _():
            j = i - 3
            for par in (0, 1):
                q = 2 * j + par
                g3(q, True).wait_recv()
                xbuf[:, par * HALF:(par + 1) * HALF] = (
                    gath[q].astype(f32).reshape(total, HALF).astype(bf16)
                )
            for c in wcopies(j):
                c.wait()

            def tile(n, c2):
                at = pl.ds(pl.multiple_of(n * TILE, TILE), TILE)
                acc_g[:, at] += jnp.dot(xbuf[...], wg[j, :, at], preferred_element_type=f32)
                acc_u[:, at] += jnp.dot(xbuf[...], wu[j, :, at], preferred_element_type=f32)
                return c2

            lax.fori_loop(0, ff // TILE, tile, 0)

        return carry

    lax.fori_loop(0, pairs + 3, gather_step, 0)
    g3(None, True).wait_recv()

    full = meta[...].astype(f32).reshape(total, LANES)
    cnt_ref[...] = jnp.broadcast_to(jnp.sum(full, axis=0, keepdims=True), cnt_ref.shape)
    mine = gx * nz + z
    lane2 = lax.broadcasted_iota(jnp.int32, (total, LANES), 1)
    weight = jnp.sum(jnp.where(lane2 == mine, full, 0.0), axis=1, keepdims=True)

    for n in range(ff // TILE):
        at = slice(n * TILE, (n + 1) * TILE)
        g = acc_g[:, at]
        hid[:, at] = (g / (1.0 + jnp.exp(-g)) * acc_u[:, at] * weight).astype(bf16)

    def c1(q):
        return remote(s0.at[q, 1 - core], r1.at[q], c1_s.at[q], c1_r.at[q], sib)

    def c2(q, par):
        if par == 0:
            src, dev = s1.at[q, 1 - y], ypeer
        else:
            src, dev = s1.at[q, :, 1 - x], xpeer
        return remote(src, r2.at[q], c2_s.at[q], c2_r.at[q], dev)

    def c3(q, par):
        if par == 0:
            src, dev = s2.at[q, 1 - x], xpeer
        else:
            src, dev = s2.at[q, 1 - y], ypeer
        return remote(src, r3.at[q], c3_s.at[q], c3_r.at[q], dev)

    def c4(q, d):
        return remote(
            s3.at[q, lax.rem(z + d, nz)], r4.at[q, d - 1],
            c4_s.at[q, d - 1], c4_r.at[q, d - 1], zpeer(d),
        )

    def add(a, b):
        return (a.astype(f32) + b.astype(f32)).astype(bf16)

    def reduce_step(i, carry):
        @pl.when(i < pairs)
        def _():
            dcopy(i).wait()
            for n in range(PAIR // TILE):
                part = jnp.dot(
                    hid[...], wd[i, :, n * TILE:(n + 1) * TILE], preferred_element_type=f32
                )
                lo = n * TILE % HALF
                s0[2 * i + n * TILE // HALF, :, :, :, :, :, lo:lo + TILE] = part.reshape(
                    s0.shape[1:-1] + (TILE,)
                ).astype(bf16)
            for par in (0, 1):
                c1(2 * i + par).start()

        @pl.when((i >= 1) & (i < pairs + 1))
        def _():
            for par in (0, 1):
                q = 2 * (i - 1) + par
                c1(q).wait_recv()
                s1[q] = add(s0[q, core], r1[q])
                c2(q, par).start()

        @pl.when((i >= 2) & (i < pairs + 2))
        def _():
            for par in (0, 1):
                q = 2 * (i - 2) + par
                c2(q, par).wait_recv()
                s2[q] = add(s1[q, y] if par == 0 else s1[q, :, x], r2[q])
                c3(q, par).start()

        @pl.when((i >= 3) & (i < pairs + 3))
        def _():
            for par in (0, 1):
                q = 2 * (i - 3) + par
                c3(q, par).wait_recv()
                s3[q] = add(s2[q, x] if par == 0 else s2[q, y], r3[q])
                for d in range(1, nz):
                    c4(q, d).start()

        @pl.when(i >= 4)
        def _():
            for par in (0, 1):
                q = 2 * (i - 4) + par
                done = s3[q, z].astype(f32)
                for d in range(1, nz):
                    c4(q, d).wait_recv()
                    done = done + r4[q, d - 1].astype(f32)
                out_ref[:, cols(q)] = done.astype(bf16)

        return carry

    lax.fori_loop(0, pairs + 4, reduce_step, 0)

    def drain(i, carry):
        for par in (0, 1):
            q = 2 * i + par
            for d in range(1, nz):
                gz(q, d).wait_send()
                c4(q, d).wait_send()
            g1(q, par).wait_send()
            g2(q, par).wait_send()
            g3(q).wait_send()
            c1(q).wait_send()
            c2(q, par).wait_send()
            c3(q, par).wait_send()
        return carry

    lax.fori_loop(0, pairs, drain, 0)
    for d in range(1, nz):
        gz(None, d).wait_send()
    g1(None, 0).wait_send()
    g2(None, 0).wait_send()
    g3(None).wait_send()


def fused_body(
    tokens, expert_ids, slot_ids, route_weight, gate_weight, up_weight, down_weight, expert_bias
):
    nz = lax.axis_size("gy")
    experts = lax.axis_size("gx") * nz
    devices = experts * lax.axis_size("gz")
    rows, width = tokens.shape
    ff = gate_weight.shape[2]
    total = rows * devices
    pairs = width // PAIR
    chunks = 2 * pairs
    bf16, f32 = jnp.bfloat16, jnp.float32
    vm = pl.BlockSpec(memory_space=pltpu.VMEM)
    hbm = pl.BlockSpec(memory_space=pl.ANY)
    dma = pltpu.SemaphoreType.DMA
    blk = (nz, rows, HALF)
    combined, counts = pl.pallas_call(
        layer_kernel,
        out_shape=(
            jax.ShapeDtypeStruct((rows, width), bf16),
            jax.ShapeDtypeStruct((8, LANES), f32),
        ),
        in_specs=[vm, vm, vm, hbm, hbm, hbm],
        out_specs=(vm, vm),
        scratch_shapes=[
            pltpu.VMEM((pairs, PAIR, ff), bf16),
            pltpu.VMEM((pairs, PAIR, ff), bf16),
            pltpu.VMEM((pairs, ff, PAIR), bf16),
            pltpu.VMEM((chunks, 2, 2, 2) + blk, bf16),
            pltpu.VMEM((2, 2, 2, nz, rows, LANES), bf16),
            pltpu.VMEM((total, PAIR), bf16),
            pltpu.VMEM((total, ff), f32),
            pltpu.VMEM((total, ff), f32),
            pltpu.VMEM((total, ff), bf16),
            pltpu.VMEM((chunks, 2, 2, 2) + blk, bf16),
            pltpu.VMEM((chunks, 2, 2) + blk, bf16),
            pltpu.VMEM((chunks, 2, 2) + blk, bf16),
            pltpu.VMEM((chunks, 2) + blk, bf16),
            pltpu.VMEM((chunks, 2) + blk, bf16),
            pltpu.VMEM((chunks,) + blk, bf16),
            pltpu.VMEM((chunks,) + blk, bf16),
            pltpu.VMEM((chunks, nz - 1, rows, HALF), bf16),
            dma((4, chunks)),
            dma((chunks + 1, nz - 1)), dma((chunks + 1, nz - 1)),
            dma((chunks + 1,)), dma((chunks + 1,)),
            dma((chunks + 1,)), dma((chunks + 1,)),
            dma((chunks + 1,)), dma((chunks + 1,)),
            dma((chunks,)), dma((chunks,)),
            dma((chunks,)), dma((chunks,)),
            dma((chunks,)), dma((chunks,)),
            dma((chunks, nz - 1)), dma((chunks, nz - 1)),
        ],
        compiler_params=pltpu.CompilerParams(
            collective_id=0, has_side_effects=True, vmem_limit_bytes=67043328
        ),
        name="expert_layer",
    )(tokens, expert_ids, route_weight, gate_weight, up_weight, down_weight)
    expert_load = counts[0, experts:2 * experts].astype(jnp.int32)
    mean_load = total * expert_ids.shape[1] // experts
    new_bias = expert_bias + bias_rate * jnp.sign((mean_load - expert_load).astype(f32))
    return (combined, expert_load, new_bias)


def body(tokens, *rest):
    sizes = (lax.axis_size("gx"), lax.axis_size("gz"))
    fits = sizes == (4, 2) and tokens.shape[0] == 8 and tokens.shape[1] % PAIR == 0
    return (fused_body if fits else slot_body)(tokens, *rest)


def solution(mesh):
    return jax.shard_map(
        body,
        mesh=mesh,
        in_specs=(
            P(("gx", "gy", "gz"), None),
            P(("gx", "gy", "gz"), None),
            P(("gx", "gy", "gz"), None),
            P(("gx", "gy", "gz"), None),
            P(("gx", "gy"), None, "gz"),
            P(("gx", "gy"), None, "gz"),
            P(("gx", "gy"), "gz", None),
            P(),
        ),
        out_specs=(P(("gx", "gy", "gz"), None), P(), P()),
        check_vma=False,
    )
```

```python
import jax
import jax.numpy as jnp
from jax import lax
from jax.experimental import pallas as pl
from jax.experimental.pallas import tpu as pltpu
from jax.sharding import PartitionSpec as P

PLACE_LIMIT = 8


bias_rate = 0.001


def pack_rows(targets, tokens, row_total):
    selection = jnp.any(
        targets[None, :, :] == jnp.arange(row_total, dtype=jnp.int32)[:, None, None], axis=2
    )
    return jnp.dot(
        selection.astype(jnp.bfloat16), tokens, preferred_element_type=jnp.float32
    ).astype(jnp.bfloat16)


def send_rows(buffer):
    arrived = lax.all_to_all(buffer, ("gx", "gy", "gz"), split_axis=1, concat_axis=1, tiled=True)
    return arrived


def return_rows(buffer):
    arrived = lax.all_to_all(buffer, ("gx", "gy", "gz"), split_axis=1, concat_axis=1, tiled=True)
    return arrived


def slot_body(
    tokens, expert_ids, slot_ids, route_weight, gate_weight, up_weight, down_weight, expert_bias
):
    experts = lax.axis_size("gx") * lax.axis_size("gy")
    gz_parts = lax.axis_size("gz")
    devices = experts * gz_parts
    tok_rows, model_width = tokens.shape
    route_count = expert_ids.shape[1]
    capacity = PLACE_LIMIT
    slot_share = capacity // gz_parts
    expert_index = jnp.arange(experts, dtype=jnp.int32)
    local_hits = jnp.sum((expert_ids[:, :, None] == expert_index).astype(jnp.int32), axis=(0, 1))
    expert_load = lax.psum(local_hits, ("gx", "gy", "gz"))
    mean_load = tok_rows * devices * route_count // experts
    new_bias = expert_bias + bias_rate * jnp.sign((mean_load - expert_load).astype(jnp.float32))
    back_rows = slot_ids % slot_share * devices + expert_ids * gz_parts + slot_ids // slot_share
    packed = pack_rows(slot_ids * experts + expert_ids, tokens, capacity * experts)
    repeated = jnp.broadcast_to(
        packed.reshape(capacity, experts, 1, model_width),
        (capacity, experts, gz_parts, model_width),
    )
    received = send_rows(repeated.reshape(capacity, devices, model_width))
    gate_mat = gate_weight[0]
    up_mat = up_weight[0]
    down_mat = down_weight[0]
    flat_rows = received.reshape(slot_share * lax.axis_size("gz") * devices, model_width)
    gate_act = jnp.dot(flat_rows, gate_mat, preferred_element_type=jnp.float32)
    up_act = jnp.dot(flat_rows, up_mat, preferred_element_type=jnp.float32)
    hidden = (jax.nn.silu(gate_act) * up_act).astype(jnp.bfloat16)
    partial_out = jnp.dot(hidden, down_mat, preferred_element_type=jnp.float32)
    summed = lax.psum_scatter(
        partial_out.reshape(slot_share * lax.axis_size("gz"), devices, model_width).astype(
            jnp.bfloat16
        ),
        "gz",
        scatter_dimension=0,
        tiled=True,
    )
    answers = return_rows(summed)
    flat_answers = answers.reshape(slot_share * devices, model_width)
    spread = jnp.where(
        back_rows[:, :, None] == jnp.arange(slot_share * devices, dtype=jnp.int32),
        route_weight.astype(jnp.float32)[:, :, None],
        0.0,
    )
    mixing = jnp.sum(spread, axis=1).astype(jnp.bfloat16)
    combined = jnp.dot(mixing, flat_answers, preferred_element_type=jnp.float32).astype(
        jnp.bfloat16
    )
    return (combined, expert_load, new_bias)


PAIR = 1792
HALF = PAIR // 2
TILE = 256
LANES = 128
MESH = pl.DeviceIdType.MESH


def layer_kernel(
    tok_ref, ids_ref, rw_ref, wg_hbm, wu_hbm, wd_hbm,
    out_ref, cnt_ref,
    wg, wu, wd, gath, meta, xbuf, acc_g, acc_u, hid,
    s0, r1, s1, r2, s2, r3, s3, r4,
    w_sem, gz_s, gz_r, g1_s, g1_r, g2_s, g2_r, g3_s, g3_r,
    c1_s, c1_r, c2_s, c2_r, c3_s, c3_r, c4_s, c4_r,
):
    f32, bf16 = jnp.float32, jnp.bfloat16
    gx, z, x = lax.axis_index("gx"), lax.axis_index("gy"), lax.axis_index("gz")
    nz = lax.axis_size("gy")
    experts = lax.axis_size("gx") * nz
    y, core = gx // 2, gx % 2
    rows = tok_ref.shape[0]
    total = gath.shape[1] * gath.shape[2] * gath.shape[3] * nz * rows
    ff = hid.shape[1]
    pairs = gath.shape[0] // 2
    sib = (y * 2 + (1 - core), z, x)
    ypeer = ((1 - y) * 2 + core, z, x)
    xpeer = (gx, z, 1 - x)

    def zpeer(d):
        return (gx, lax.rem(z + d, nz), x)

    def wcopies(j):
        span = pl.ds(pl.multiple_of(j * PAIR, PAIR), PAIR)
        return (
            pltpu.make_async_copy(wg_hbm.at[0, span, :], wg.at[j], w_sem.at[0, j]),
            pltpu.make_async_copy(wu_hbm.at[0, span, :], wu.at[j], w_sem.at[1, j]),
        )

    def dcopy(j):
        span = pl.ds(pl.multiple_of(j * PAIR, PAIR), PAIR)
        return pltpu.make_async_copy(wd_hbm.at[0, :, span], wd.at[j], w_sem.at[2, j])

    def start_gate(j, carry):
        for c in wcopies(j):
            c.start()
        return carry

    def start_down(j, carry):
        dcopy(j).start()
        return carry

    lax.fori_loop(0, pairs, start_gate, 0)
    lax.fori_loop(0, pairs, start_down, 0)

    ids = ids_ref[...]
    rw = rw_ref[...].astype(f32)
    lane = lax.broadcasted_iota(jnp.int32, (rows, LANES), 1)
    table = jnp.zeros((rows, LANES), f32)
    for k in range(ids.shape[1]):
        col = ids[:, k:k + 1]
        table = table + jnp.where(lane == col, rw[:, k:k + 1], 0.0)
        table = table + jnp.where(lane == col + experts, 1.0, 0.0)
    meta[core, y, x, z] = table.astype(bf16)

    barrier = pltpu.get_barrier_semaphore()
    peers = [sib, ypeer, xpeer] + [zpeer(d) for d in range(1, nz)]
    for peer in peers:
        pl.semaphore_signal(barrier, inc=1, device_id=peer, device_id_type=MESH)
    pl.semaphore_wait(barrier, len(peers))

    def remote(src, dst, ssem, rsem, dev):
        return pltpu.make_async_remote_copy(
            src_ref=src, dst_ref=dst, send_sem=ssem, recv_sem=rsem,
            device_id=dev, device_id_type=MESH,
        )

    last = pairs * 2

    def view(q):
        return meta if q is None else gath.at[q]

    def semi(q):
        return last if q is None else q

    def cols(q):
        return pl.ds(pl.multiple_of(q * HALF, HALF), HALF)

    def gz(q, d, inn=False):
        buf = view(q)
        own = buf.at[core, y, x, z]
        src = meta.at[core, y, x, z] if q is None else tok_ref.at[:, cols(q)]
        dst = buf.at[core, y, x, lax.rem(z - d + nz, nz)] if inn else own
        return remote(src, dst, gz_s.at[semi(q), d - 1], gz_r.at[semi(q), d - 1], zpeer(d))

    def own_copy(q):
        return pltpu.make_async_copy(
            tok_ref.at[:, cols(q)], gath.at[q, core, y, x, z], w_sem.at[3, q]
        )

    def g1(q, par, inn=False):
        buf = view(q)
        src = buf.at[core, y, x]
        if par == 0:
            dst = buf.at[core, y, 1 - x] if inn else src
            dev = xpeer
        else:
            dst = buf.at[core, 1 - y, x] if inn else src
            dev = ypeer
        return remote(src, dst, g1_s.at[semi(q)], g1_r.at[semi(q)], dev)

    def g2(q, par, inn=False):
        buf = view(q)
        if par == 0:
            src = buf.at[core, y]
            dst = buf.at[core, 1 - y] if inn else src
            dev = ypeer
        else:
            src = buf.at[core, :, x]
            dst = buf.at[core, :, 1 - x] if inn else src
            dev = xpeer
        return remote(src, dst, g2_s.at[semi(q)], g2_r.at[semi(q)], dev)

    def g3(q, inn=False):
        buf = view(q)
        src = buf.at[core]
        dst = buf.at[1 - core] if inn else src
        return remote(src, dst, g3_s.at[semi(q)], g3_r.at[semi(q)], sib)

    for d in range(1, nz):
        gz(None, d).start()

    def send_z(i, carry):
        for par in (0, 1):
            q = 2 * i + par
            for d in range(1, nz):
                gz(q, d).start()
            own_copy(q).start()
        return carry

    lax.fori_loop(0, pairs, send_z, 0)

    for d in range(1, nz):
        gz(None, d, True).wait_recv()
    g1(None, 0).start()

    acc_g[...] = jnp.zeros_like(acc_g)
    acc_u[...] = jnp.zeros_like(acc_u)

    def gather_step(i, carry):
        @pl.when(i < pairs)
        def _():
            for par in (0, 1):
                q = 2 * i + par
                own_copy(q).wait()
                for d in range(1, nz):
                    gz(q, d, True).wait_recv()
                g1(q, par).start()

        @pl.when(i == 0)
        def _():
            g1(None, 0, True).wait_recv()
            g2(None, 0).start()

        @pl.when((i >= 1) & (i < pairs + 1))
        def _():
            for par in (0, 1):
                q = 2 * (i - 1) + par
                g1(q, par, True).wait_recv()
                g2(q, par).start()

        @pl.when(i == 1)
        def _():
            g2(None, 0, True).wait_recv()
            g3(None).start()

        @pl.when((i >= 2) & (i < pairs + 2))
        def _():
            for par in (0, 1):
                q = 2 * (i - 2) + par
                g2(q, par, True).wait_recv()
                g3(q).start()

        @pl.when(i >= 3)
        def _():
            j = i - 3
            for par in (0, 1):
                q = 2 * j + par
                g3(q, True).wait_recv()
                xbuf[:, par * HALF:(par + 1) * HALF] = (
                    gath[q].astype(f32).reshape(total, HALF).astype(bf16)
                )
            for c in wcopies(j):
                c.wait()

            def tile(n, c2):
                at = pl.ds(pl.multiple_of(n * TILE, TILE), TILE)
                acc_g[:, at] += jnp.dot(xbuf[...], wg[j, :, at], preferred_element_type=f32)
                acc_u[:, at] += jnp.dot(xbuf[...], wu[j, :, at], preferred_element_type=f32)
                return c2

            lax.fori_loop(0, ff // TILE, tile, 0)

        return carry

    lax.fori_loop(0, pairs + 3, gather_step, 0)
    g3(None, True).wait_recv()

    full = meta[...].astype(f32).reshape(total, LANES)
    cnt_ref[...] = jnp.broadcast_to(jnp.sum(full, axis=0, keepdims=True), cnt_ref.shape)
    mine = gx * nz + z
    lane2 = lax.broadcasted_iota(jnp.int32, (total, LANES), 1)
    weight = jnp.sum(jnp.where(lane2 == mine, full, 0.0), axis=1, keepdims=True)

    for n in range(ff // TILE):
        at = slice(n * TILE, (n + 1) * TILE)
        g = acc_g[:, at]
        hid[:, at] = (g / (1.0 + jnp.exp(-g)) * acc_u[:, at] * weight).astype(bf16)

    def c1(q):
        return remote(s0.at[q, 1 - core], r1.at[q], c1_s.at[q], c1_r.at[q], sib)

    def c2(q, par):
        if par == 0:
            src, dev = s1.at[q, 1 - y], ypeer
        else:
            src, dev = s1.at[q, :, 1 - x], xpeer
        return remote(src, r2.at[q], c2_s.at[q], c2_r.at[q], dev)

    def c3(q, par):
        if par == 0:
            src, dev = s2.at[q, 1 - x], xpeer
        else:
            src, dev = s2.at[q, 1 - y], ypeer
        return remote(src, r3.at[q], c3_s.at[q], c3_r.at[q], dev)

    def c4(q, d):
        return remote(
            s3.at[q, lax.rem(z + d, nz)], r4.at[q, d - 1],
            c4_s.at[q, d - 1], c4_r.at[q, d - 1], zpeer(d),
        )

    def add(a, b):
        return (a.astype(f32) + b.astype(f32)).astype(bf16)

    def reduce_step(i, carry):
        @pl.when(i < pairs)
        def _():
            dcopy(i).wait()
            for par in (0, 1):
                part = jnp.dot(
                    hid[...], wd[i, :, par * HALF:(par + 1) * HALF], preferred_element_type=f32
                )
                s0[2 * i + par] = part.reshape(s0.shape[1:-1] + (HALF,)).astype(bf16)
                c1(2 * i + par).start()

        @pl.when((i >= 1) & (i < pairs + 1))
        def _():
            for par in (0, 1):
                q = 2 * (i - 1) + par
                c1(q).wait_recv()
                s1[q] = add(s0[q, core], r1[q])
                c2(q, par).start()

        @pl.when((i >= 2) & (i < pairs + 2))
        def _():
            for par in (0, 1):
                q = 2 * (i - 2) + par
                c2(q, par).wait_recv()
                s2[q] = add(s1[q, y] if par == 0 else s1[q, :, x], r2[q])
                c3(q, par).start()

        @pl.when((i >= 3) & (i < pairs + 3))
        def _():
            for par in (0, 1):
                q = 2 * (i - 3) + par
                c3(q, par).wait_recv()
                s3[q] = add(s2[q, x] if par == 0 else s2[q, y], r3[q])
                for d in range(1, nz):
                    c4(q, d).start()

        @pl.when(i >= 4)
        def _():
            for par in (0, 1):
                q = 2 * (i - 4) + par
                done = s3[q, z].astype(f32)
                for d in range(1, nz):
                    c4(q, d).wait_recv()
                    done = done + r4[q, d - 1].astype(f32)
                out_ref[:, cols(q)] = done.astype(bf16)

        return carry

    lax.fori_loop(0, pairs + 4, reduce_step, 0)

    def drain(i, carry):
        for par in (0, 1):
            q = 2 * i + par
            for d in range(1, nz):
                gz(q, d).wait_send()
                c4(q, d).wait_send()
            g1(q, par).wait_send()
            g2(q, par).wait_send()
            g3(q).wait_send()
            c1(q).wait_send()
            c2(q, par).wait_send()
            c3(q, par).wait_send()
        return carry

    lax.fori_loop(0, pairs, drain, 0)
    for d in range(1, nz):
        gz(None, d).wait_send()
    g1(None, 0).wait_send()
    g2(None, 0).wait_send()
    g3(None).wait_send()


def fused_body(
    tokens, expert_ids, slot_ids, route_weight, gate_weight, up_weight, down_weight, expert_bias
):
    nz = lax.axis_size("gy")
    experts = lax.axis_size("gx") * nz
    devices = experts * lax.axis_size("gz")
    rows, width = tokens.shape
    ff = gate_weight.shape[2]
    total = rows * devices
    pairs = width // PAIR
    chunks = 2 * pairs
    bf16, f32 = jnp.bfloat16, jnp.float32
    vm = pl.BlockSpec(memory_space=pltpu.VMEM)
    hbm = pl.BlockSpec(memory_space=pl.ANY)
    dma = pltpu.SemaphoreType.DMA
    blk = (nz, rows, HALF)
    combined, counts = pl.pallas_call(
        layer_kernel,
        out_shape=(
            jax.ShapeDtypeStruct((rows, width), bf16),
            jax.ShapeDtypeStruct((8, LANES), f32),
        ),
        in_specs=[vm, vm, vm, hbm, hbm, hbm],
        out_specs=(vm, vm),
        scratch_shapes=[
            pltpu.VMEM((pairs, PAIR, ff), bf16),
            pltpu.VMEM((pairs, PAIR, ff), bf16),
            pltpu.VMEM((pairs, ff, PAIR), bf16),
            pltpu.VMEM((chunks, 2, 2, 2) + blk, bf16),
            pltpu.VMEM((2, 2, 2, nz, rows, LANES), bf16),
            pltpu.VMEM((total, PAIR), bf16),
            pltpu.VMEM((total, ff), f32),
            pltpu.VMEM((total, ff), f32),
            pltpu.VMEM((total, ff), bf16),
            pltpu.VMEM((chunks, 2, 2, 2) + blk, bf16),
            pltpu.VMEM((chunks, 2, 2) + blk, bf16),
            pltpu.VMEM((chunks, 2, 2) + blk, bf16),
            pltpu.VMEM((chunks, 2) + blk, bf16),
            pltpu.VMEM((chunks, 2) + blk, bf16),
            pltpu.VMEM((chunks,) + blk, bf16),
            pltpu.VMEM((chunks,) + blk, bf16),
            pltpu.VMEM((chunks, nz - 1, rows, HALF), bf16),
            dma((4, chunks)),
            dma((chunks + 1, nz - 1)), dma((chunks + 1, nz - 1)),
            dma((chunks + 1,)), dma((chunks + 1,)),
            dma((chunks + 1,)), dma((chunks + 1,)),
            dma((chunks + 1,)), dma((chunks + 1,)),
            dma((chunks,)), dma((chunks,)),
            dma((chunks,)), dma((chunks,)),
            dma((chunks,)), dma((chunks,)),
            dma((chunks, nz - 1)), dma((chunks, nz - 1)),
        ],
        compiler_params=pltpu.CompilerParams(
            collective_id=0, has_side_effects=True, vmem_limit_bytes=67043328
        ),
        name="expert_layer",
    )(tokens, expert_ids, route_weight, gate_weight, up_weight, down_weight)
    expert_load = counts[0, experts:2 * experts].astype(jnp.int32)
    mean_load = total * expert_ids.shape[1] // experts
    new_bias = expert_bias + bias_rate * jnp.sign((mean_load - expert_load).astype(f32))
    return (combined, expert_load, new_bias)


def body(tokens, *rest):
    sizes = (lax.axis_size("gx"), lax.axis_size("gz"))
    fits = sizes == (4, 2) and tokens.shape[0] == 8 and tokens.shape[1] % PAIR == 0
    return (fused_body if fits else slot_body)(tokens, *rest)


def solution(mesh):
    return jax.shard_map(
        body,
        mesh=mesh,
        in_specs=(
            P(("gx", "gy", "gz"), None),
            P(("gx", "gy", "gz"), None),
            P(("gx", "gy", "gz"), None),
            P(("gx", "gy", "gz"), None),
            P(("gx", "gy"), None, "gz"),
            P(("gx", "gy"), None, "gz"),
            P(("gx", "gy"), "gz", None),
            P(),
        ),
        out_specs=(P(("gx", "gy", "gz"), None), P(), P()),
        check_vma=False,
    )
```
